8 devices in a mesh: dp: 8 (over z, y, x, core).
Axes of the slice: x: 2, y: 2, z: 1, core: 2. Of those that a mesh axis runs over, the one named last changes fastest.
Arguments:
- token_ids: int32 [48, 512], P('dp')
- target_ids: int32 [48, 512], P('dp')
- st_wte: float32 [3, 50257, 256], P(None, None, 'dp')
- st_wpe: float32 [3, 2050, 256], P(None, None, 'dp')
- st_qkv: float32 [3, 2, 256, 3, 16, 16], P(None, None, 'dp')
- st_proj: float32 [3, 2, 16, 16, 256], P(None, None, None, None, 'dp')
- st_up: float32 [3, 2, 256, 1024], P(None, None, 'dp')
- st_down: float32 [3, 2, 1024, 256], P(None, None, 'dp')
- st_vec: float32 [3, 2, 3328], P(None, None, 'dp')
- st_lnf: float32 [3, 2, 256], P(None, None, 'dp')
Outputs:
- output 1: float32 [], replicated
- output 2: float32 [3, 50257, 256], P(None, None, 'dp')
- output 3: float32 [3, 2050, 256], P(None, None, 'dp')
- output 4: float32 [3, 2, 256, 3, 16, 16], P(None, None, 'dp')
- output 5: float32 [3, 2, 16, 16, 256], P(None, None, None, None, 'dp')
- output 6: float32 [3, 2, 256, 1024], P(None, None, 'dp')
- output 7: float32 [3, 2, 1024, 256], P(None, None, 'dp')
- output 8: float32 [3, 2, 3328], P(None, None, 'dp')
- output 9: float32 [3, 2, 256], P(None, None, 'dp')
All inputs are finite; a program needn't handle non-finite values.
Results may differ from the reference program's by a relative error of at most 0.00251365.
Values are sent between devices in bfloat16 or wider.
A program may use at most 1 GiB of HBM per device.

```python
import jax
import jax.numpy as jnp
from jax import lax

NUM_DEVICES = 8
BATCH_DEV = 6
SEQ_LEN = 512
D_MODEL = 256
NUM_HEADS = 16
HEAD_DIM = 16
FF_DIM = 1024
VOCAB_SIZE = 50257
MAX_POS = 2048
NUM_LAYERS = 2
ADAM_STEP = 10
HOT_IDS = 16

TOTAL_ROWS = NUM_DEVICES * BATCH_DEV
POS_ROWS = MAX_POS + 2
VEC_LEN = 9 * D_MODEL + FF_DIM
INV_TOKENS = 1.0 / (TOTAL_ROWS * SEQ_LEN)
SCORE_SCALE = HEAD_DIM ** -0.5
NORM_EPS = 1e-5
LEARN_RATE = 3e-3
BETA_ONE = 0.9
BETA_TWO = 0.95
ADAM_EPS = 1e-8
WEIGHT_DECAY = 0.1
CLIP_NORM = 1.0
MOM_SCALE = 2e-6
DECAYS = (WEIGHT_DECAY,) * 6 + (0.0, 0.0)


def draw_tokens(base_key):
    k_ids, k_wide, k_hot, k_pick, k_flip = jax.random.split(base_key, 5)
    tok_grid = (TOTAL_ROWS, SEQ_LEN)
    token_ids = jax.random.randint(k_ids, tok_grid, 0, VOCAB_SIZE, jnp.int32)
    token_ids = token_ids.at[0, 0].set(VOCAB_SIZE - 1).at[0, 1].set(0)
    hot_table = jax.random.randint(k_hot, (HOT_IDS,), 0, VOCAB_SIZE, jnp.int32)
    hot_pick = hot_table[jax.random.randint(k_pick, tok_grid, 0, HOT_IDS, jnp.int32)]
    wide_pick = jax.random.randint(k_wide, tok_grid, 0, VOCAB_SIZE, jnp.int32)
    coin_flip = jax.random.randint(k_flip, tok_grid, 0, 2, jnp.int32)
    target_ids = jnp.where(coin_flip == 1, hot_pick, wide_pick)
    target_ids = target_ids.at[0, 0].set(VOCAB_SIZE - 1).at[0, 1].set(0)
    return token_ids, target_ids


def draw_state(base_key, dims, center, scale):
    k_par, k_mom, k_sec = jax.random.split(base_key, 3)
    master = center + scale * jax.random.normal(k_par, dims, jnp.float32)
    moment = MOM_SCALE * jax.random.normal(k_mom, dims, jnp.float32)
    second = (MOM_SCALE * jax.random.uniform(k_sec, dims, jnp.float32, 0.5, 1.5)) ** 2
    return jnp.stack([master, moment, second])


def setup_inputs(seed: int = 0) -> dict:
    key_list = jax.random.split(jax.random.key(seed), 9)
    token_ids, target_ids = draw_tokens(key_list[0])
    d_scale = D_MODEL ** -0.5
    vec_center = jnp.concatenate([jnp.zeros((5 * D_MODEL + FF_DIM,), jnp.float32), jnp.ones((D_MODEL,), jnp.float32), jnp.zeros((D_MODEL,), jnp.float32), jnp.ones((D_MODEL,), jnp.float32), jnp.zeros((D_MODEL,), jnp.float32)])
    lnf_center = jnp.array([[1.0], [0.0]], jnp.float32)
    lnf_scale = jnp.array([[0.2], [1.0]], jnp.float32)
    return dict(
        token_ids=token_ids,
        target_ids=target_ids,
        st_wte=draw_state(key_list[1], (VOCAB_SIZE, D_MODEL), 0.0, d_scale),
        st_wpe=draw_state(key_list[2], (POS_ROWS, D_MODEL), 0.0, d_scale),
        st_qkv=draw_state(key_list[3], (NUM_LAYERS, D_MODEL, 3, NUM_HEADS, HEAD_DIM), 0.0, d_scale),
        st_proj=draw_state(key_list[4], (NUM_LAYERS, NUM_HEADS, HEAD_DIM, D_MODEL), 0.0, d_scale),
        st_up=draw_state(key_list[5], (NUM_LAYERS, D_MODEL, FF_DIM), 0.0, d_scale),
        st_down=draw_state(key_list[6], (NUM_LAYERS, FF_DIM, D_MODEL), 0.0, FF_DIM ** -0.5),
        st_vec=draw_state(key_list[7], (NUM_LAYERS, VEC_LEN), vec_center, 0.2),
        st_lnf=draw_state(key_list[8], (2, D_MODEL), lnf_center, lnf_scale),
    )


def layer_norm(residual, gain, bias):
    mean_val = jnp.mean(residual, axis=-1, keepdims=True)
    centered = residual - mean_val
    variance = jnp.mean(centered * centered, axis=-1, keepdims=True)
    return centered * lax.rsqrt(variance + NORM_EPS) * gain.astype(jnp.float32) + bias.astype(jnp.float32)


def block(residual, qkv_w, proj_w, up_w, down_w, layer_vec):
    seq_len = residual.shape[0]
    offset = 4 * D_MODEL + FF_DIM
    ln_par = layer_vec[offset + D_MODEL:].reshape(4, D_MODEL)
    normed_in = layer_norm(residual, ln_par[0], ln_par[1]).astype(jnp.bfloat16)
    qkv_all = jnp.dot(normed_in, qkv_w.reshape(D_MODEL, 3 * D_MODEL), preferred_element_type=jnp.float32) + layer_vec[:3 * D_MODEL].astype(jnp.float32)
    qkv_all = qkv_all.astype(jnp.bfloat16).reshape(seq_len, 3, NUM_HEADS, HEAD_DIM).astype(jnp.float32)
    scores = jnp.einsum('qhk,shk->hqs', qkv_all[:, 0], qkv_all[:, 1]) * SCORE_SCALE
    causal = jnp.arange(seq_len)[:, None] >= jnp.arange(seq_len)[None, :]
    scores = jnp.where(causal[None], scores, -1e30)
    attn_prob = jax.nn.softmax(scores, axis=-1).astype(jnp.bfloat16).astype(jnp.float32)
    mixed = jnp.einsum('hqs,shk->qhk', attn_prob, qkv_all[:, 2]).astype(jnp.bfloat16)
    residual = residual + jnp.dot(mixed.reshape(seq_len, D_MODEL), proj_w.reshape(D_MODEL, D_MODEL), preferred_element_type=jnp.float32) + layer_vec[3 * D_MODEL:4 * D_MODEL].astype(jnp.float32)
    normed_mid = layer_norm(residual, ln_par[2], ln_par[3]).astype(jnp.bfloat16)
    hidden = jax.nn.relu(jnp.dot(normed_mid, up_w, preferred_element_type=jnp.float32) + layer_vec[4 * D_MODEL:offset].astype(jnp.float32)).astype(jnp.bfloat16)
    return residual + jnp.dot(hidden, down_w, preferred_element_type=jnp.float32) + layer_vec[offset:offset + D_MODEL].astype(jnp.float32)


def sequence_loss(masters, row_ids, row_tgt):
    wte_c, wpe_c, qkv_w, proj_w, up_w, down_w, vec_all, lnf_c = [w.astype(jnp.bfloat16) for w in masters]
    residual = masters[0][row_ids].astype(jnp.bfloat16).astype(jnp.float32) + wpe_c[2:2 + SEQ_LEN].astype(jnp.float32)
    for layer in range(NUM_LAYERS):
        residual = block(residual, qkv_w[layer], proj_w[layer], up_w[layer], down_w[layer], vec_all[layer])
    normed = layer_norm(residual, lnf_c[0], lnf_c[1]).astype(jnp.bfloat16)
    logits = jnp.dot(normed, wte_c.T, preferred_element_type=jnp.float32)
    picked = jnp.take_along_axis(logits, row_tgt[:, None], axis=-1)[:, 0]
    return jnp.sum(jax.nn.logsumexp(logits, axis=-1) - picked) * INV_TOKENS


def adam_update(state, grad, decay):
    moment = BETA_ONE * state[1] + (1.0 - BETA_ONE) * grad
    second = BETA_TWO * state[2] + (1.0 - BETA_TWO) * grad * grad
    m_hat = moment / (1.0 - BETA_ONE ** ADAM_STEP)
    v_hat = second / (1.0 - BETA_TWO ** ADAM_STEP)
    master = state[0] * (1.0 - LEARN_RATE * decay) - LEARN_RATE * m_hat / (jnp.sqrt(v_hat) + ADAM_EPS)
    return jnp.stack([master, moment, second])


def reference(token_ids, target_ids, st_wte, st_wpe, st_qkv, st_proj, st_up, st_down, st_vec, st_lnf):
    states = (st_wte, st_wpe, st_qkv, st_proj, st_up, st_down, st_vec, st_lnf)
    masters = tuple(state[0] for state in states)

    def row_step(carry, row):
        grad_acc, loss_acc = carry
        row_loss, row_grad = jax.value_and_grad(sequence_loss)(masters, row[0], row[1])
        return (jax.tree.map(jnp.add, grad_acc, row_grad), loss_acc + row_loss), None

    init_carry = (tuple(jnp.zeros_like(w) for w in masters), jnp.zeros((), jnp.float32))
    (grads, loss), _ = lax.scan(row_step, init_carry, (token_ids, target_ids))
    grad_norm = jnp.sqrt(sum(jnp.sum(g * g) for g in grads))
    clip_coef = jnp.minimum(1.0, CLIP_NORM / (grad_norm + 1e-6))
    new_wte, new_wpe, new_qkv, new_proj, new_up, new_down, new_vec, new_lnf = [adam_update(state, g * clip_coef, decay) for state, g, decay in zip(states, grads, DECAYS)]
    return (loss, new_wte, new_wpe, new_qkv, new_proj, new_up, new_down, new_vec, new_lnf)
```

```python
import functools

import jax
import jax.numpy as jnp
from jax import lax
from jax.experimental import pallas as pl
from jax.experimental.pallas import tpu as pltpu
from jax.sharding import PartitionSpec as P

NORM_EPS = 1e-5
LEARN_RATE = 3e-3
BETA_ONE = 0.9
BETA_TWO = 0.95
ADAM_EPS = 1e-8
WEIGHT_DECAY = 0.1
CLIP_NORM = 1.0
ADAM_STEP = 10
DECAYS = (WEIGHT_DECAY,) * 6 + (0.0, 0.0)
VOCAB_TILE = 1536
TOKEN_TILE = 3072
LSE_CHUNK = 128
GRAD_CHUNK = 256
N_ACC = 8
HEADS_STEP = 2
LOWEST = -3.0e38
BIG_VMEM = 60 * 1024 * 1024
F32 = jnp.float32
BF16 = jnp.bfloat16


def layer_norm(residual, gain, bias):
    mean_val = jnp.mean(residual, axis=-1, keepdims=True)
    centered = residual - mean_val
    variance = jnp.mean(centered * centered, axis=-1, keepdims=True)
    return centered * lax.rsqrt(variance + NORM_EPS) * gain.astype(F32) + bias.astype(F32)


def dot(a, b):
    return jnp.dot(a, b, preferred_element_type=F32)


def attn_fwd_kernel(qkv_ref, o_ref, lse_ref, qt_ref, vt_ref, ot_ref, *, seq, dm, hd):
    qt_ref[...] = (qkv_ref[0, :, :dm] * jnp.asarray(hd ** -0.5, BF16)).T
    vt_ref[...] = qkv_ref[0, :, 2 * dm:].T
    half = seq // 2
    per = 128 // hd
    lo, hi = slice(0, half), slice(half, seq)
    row_head = lax.broadcasted_iota(jnp.int32, (128, seq), 0) // hd
    keep = lax.broadcasted_iota(jnp.int32, (half, half), 0) <= lax.broadcasted_iota(jnp.int32, (half, half), 1)
    for slab in range(dm // 128):
        base = slab * 128

        @pl.loop(0, per // HEADS_STEP)
        def _(i):
            todo = []
            for j in range(HEADS_STEP):
                hh = i * HEADS_STEP + j
                qm = jnp.where(row_head == hh, qt_ref[base:base + 128, :], jnp.zeros((), BF16))
                k_lo = qkv_ref[0, lo, dm + base:dm + base + 128]
                k_hi = qkv_ref[0, hi, dm + base:dm + base + 128]
                both = dot(k_lo, qm)
                diag = dot(k_hi, qm[:, hi])
                todo.append((hh, both[:, lo], both[:, hi], diag))
            for hh, s00, s01, s11 in todo:
                rows = pl.ds(pl.multiple_of(base + hh * hd, hd), hd)
                stat = pl.ds(slab * per + hh, 1)
                s00 = jnp.where(keep, s00, -1e30)
                s11 = jnp.where(keep, s11, -1e30)
                m0 = jnp.max(s00, axis=0, keepdims=True)
                e00 = jnp.exp(s00 - m0)
                l0 = jnp.sum(e00, axis=0, keepdims=True)
                m1 = jnp.maximum(jnp.max(s01, axis=0, keepdims=True), jnp.max(s11, axis=0, keepdims=True))
                e01 = jnp.exp(s01 - m1)
                e11 = jnp.exp(s11 - m1)
                l1 = jnp.sum(e01, axis=0, keepdims=True) + jnp.sum(e11, axis=0, keepdims=True)
                inv0, inv1 = 1.0 / l0, 1.0 / l1
                p00 = (e00 * inv0).astype(BF16)
                p01 = (e01 * inv1).astype(BF16)
                p11 = (e11 * inv1).astype(BF16)
                ot_ref[rows, lo] = dot(vt_ref[rows, lo], p00)
                ot_ref[rows, hi] = dot(vt_ref[rows, lo], p01) + dot(vt_ref[rows, hi], p11)
                lse_ref[0, stat, lo] = m0 + jnp.log(l0)
                lse_ref[0, stat, hi] = m1 + jnp.log(l1)

    o_ref[0] = ot_ref[...].T.astype(BF16)


def attn_bwd_kernel(qkv_ref, do_ref, lse_ref, dqkv_ref, qt_ref, kt_ref, dot_ref, dqt_ref, dk_ref, dv_ref, *, seq, dm, hd):
    scale = hd ** -0.5
    qt_ref[...] = (qkv_ref[0, :, :dm] * jnp.asarray(scale, BF16)).T
    kt_ref[...] = qkv_ref[0, :, dm:2 * dm].T
    dot_ref[...] = do_ref[0].T
    dk_ref[...] = jnp.zeros_like(dk_ref)
    dv_ref[...] = jnp.zeros_like(dv_ref)
    half = seq // 2
    per = 128 // hd
    lo, hi = slice(0, half), slice(half, seq)
    zero = jnp.zeros((), BF16)
    row_head = lax.broadcasted_iota(jnp.int32, (128, seq), 0) // hd
    lane_head = lax.broadcasted_iota(jnp.int32, (seq, 128), 1) // hd
    keep = lax.broadcasted_iota(jnp.int32, (half, half), 0) <= lax.broadcasted_iota(jnp.int32, (half, half), 1)
    for slab in range(dm // 128):
        base = slab * 128
        lanes = slice(base, base + 128)
        k_at = slice(dm + base, dm + base + 128)
        v_at = slice(2 * dm + base, 2 * dm + base + 128)

        @pl.loop(0, per // HEADS_STEP)
        def _(i):
            todo = []
            for j in range(HEADS_STEP):
                hh = i * HEADS_STEP + j
                qm = jnp.where(row_head == hh, qt_ref[lanes, :], zero)
                dom = jnp.where(row_head == hh, dot_ref[lanes, :], zero)
                s_lo = dot(qkv_ref[0, lo, k_at], qm)
                s_hi = dot(qkv_ref[0, hi, k_at], qm[:, hi])
                dp_lo = dot(qkv_ref[0, lo, v_at], dom)
                dp_hi = dot(qkv_ref[0, hi, v_at], dom[:, hi])
                todo.append((hh, s_lo, s_hi, dp_lo, dp_hi))
            for hh, s_lo, s_hi, dp_lo, dp_hi in todo:
                rows = pl.ds(pl.multiple_of(base + hh * hd, hd), hd)
                lse = lse_ref[0, pl.ds(slab * per + hh, 1), :]
                q_lane = jnp.where(lane_head == hh, qkv_ref[0, :, lanes], zero)
                do_lane = jnp.where(lane_head == hh, do_ref[0, :, lanes], zero)
                p00 = jnp.exp(jnp.where(keep, s_lo[:, lo], -1e30) - lse[:, lo])
                p01 = jnp.exp(s_lo[:, hi] - lse[:, hi])
                p11 = jnp.exp(jnp.where(keep, s_hi, -1e30) - lse[:, hi])
                w00, w01, w11 = p00 * dp_lo[:, lo], p01 * dp_lo[:, hi], p11 * dp_hi
                delta0 = jnp.sum(w00, axis=0, keepdims=True)
                delta1 = jnp.sum(w01, axis=0, keepdims=True) + jnp.sum(w11, axis=0, keepdims=True)
                ds_lo = jnp.concatenate([(w00 - p00 * delta0).astype(BF16), (w01 - p01 * delta1).astype(BF16)], axis=1)
                ds_hi = (w11 - p11 * delta1).astype(BF16)
                p_lo = jnp.concatenate([p00.astype(BF16), p01.astype(BF16)], axis=1)
                dv_ref[lo, lanes] += dot(p_lo, do_lane)
                dv_ref[hi, lanes] += dot(p11.astype(BF16), do_lane[hi, :])
                dk_ref[lo, lanes] += dot(ds_lo, q_lane)
                dk_ref[hi, lanes] += dot(ds_hi, q_lane[hi, :])
                dq = dot(kt_ref[rows, lo], ds_lo)
                dqt_ref[rows, lo] = dq[:, lo]
                dqt_ref[rows, hi] = dq[:, hi] + dot(kt_ref[rows, hi], ds_hi)

    dqkv_ref[0, :, :dm] = (dqt_ref[...] * scale).T.astype(BF16)
    dqkv_ref[0, :, dm:2 * dm] = (dk_ref[...] * scale).astype(BF16)
    dqkv_ref[0, :, 2 * dm:] = dv_ref[...].astype(BF16)


def attn_fwd_call(qkv, n_heads):
    batch, seq, three = qkv.shape
    dm = three // 3
    flops = 4 * batch * n_heads * seq * seq * 128
    return pl.pallas_call(
        functools.partial(attn_fwd_kernel, seq=seq, dm=dm, hd=dm // n_heads),
        grid=(batch,),
        in_specs=[pl.BlockSpec((1, seq, three), lambda b: (b, 0, 0))],
        out_specs=[pl.BlockSpec((1, seq, dm), lambda b: (b, 0, 0)), pl.BlockSpec((1, n_heads, seq), lambda b: (b, 0, 0))],
        out_shape=[jax.ShapeDtypeStruct((batch, seq, dm), BF16), jax.ShapeDtypeStruct((batch, n_heads, seq), F32)],
        scratch_shapes=[pltpu.VMEM((dm, seq), BF16), pltpu.VMEM((dm, seq), BF16), pltpu.VMEM((dm, seq), F32)],
        cost_estimate=pl.CostEstimate(flops=flops, bytes_accessed=qkv.size * 3, transcendentals=0),
        name="attn_fwd",
    )(qkv)


def attn_bwd_call(qkv, d_o, lse, n_heads):
    batch, seq, three = qkv.shape
    dm = three // 3
    flops = 10 * batch * n_heads * seq * seq * 128
    return pl.pallas_call(
        functools.partial(attn_bwd_kernel, seq=seq, dm=dm, hd=dm // n_heads),
        grid=(batch,),
        in_specs=[pl.BlockSpec((1, seq, three), lambda b: (b, 0, 0)), pl.BlockSpec((1, seq, dm), lambda b: (b, 0, 0)), pl.BlockSpec((1, n_heads, seq), lambda b: (b, 0, 0))],
        out_specs=pl.BlockSpec((1, seq, three), lambda b: (b, 0, 0)),
        out_shape=jax.ShapeDtypeStruct((batch, seq, three), BF16),
        scratch_shapes=[pltpu.VMEM((dm, seq), BF16), pltpu.VMEM((dm, seq), BF16), pltpu.VMEM((dm, seq), BF16), pltpu.VMEM((dm, seq), F32), pltpu.VMEM((seq, dm), F32), pltpu.VMEM((seq, dm), F32)],
        cost_estimate=pl.CostEstimate(flops=flops, bytes_accessed=qkv.size * 6, transcendentals=0),
        name="attn_bwd",
    )(qkv, d_o, lse)


@functools.partial(jax.custom_vjp, nondiff_argnums=(1,))
def attention(qkv, n_heads):
    return attn_fwd_call(qkv, n_heads)[0]


def attention_fwd(qkv, n_heads):
    out, lse = attn_fwd_call(qkv, n_heads)
    return out, (qkv, lse)


def attention_bwd(n_heads, saved, d_o):
    qkv, lse = saved
    return (attn_bwd_call(qkv, d_o.astype(BF16), lse, n_heads),)


attention.defvjp(attention_fwd, attention_bwd)


def block(residual, weights, n_heads):
    qkv_w, proj_w, up_w, down_w, layer_vec = weights
    d_model = residual.shape[-1]
    offset = 4 * d_model + up_w.shape[1]
    ln_par = layer_vec[offset + d_model:].reshape(4, d_model)
    normed_in = layer_norm(residual, ln_par[0], ln_par[1]).astype(BF16)
    qkv = (jnp.einsum('bsd,dn->bsn', normed_in, qkv_w, preferred_element_type=F32) + layer_vec[:3 * d_model].astype(F32)).astype(BF16)
    mixed = attention(qkv, n_heads)
    residual = residual + jnp.einsum('bsd,de->bse', mixed, proj_w, preferred_element_type=F32) + layer_vec[3 * d_model:4 * d_model].astype(F32)
    normed_mid = layer_norm(residual, ln_par[2], ln_par[3]).astype(BF16)
    hidden = jax.nn.relu(jnp.einsum('bsd,df->bsf', normed_mid, up_w, preferred_element_type=F32) + layer_vec[4 * d_model:offset].astype(F32)).astype(BF16)
    return residual + jnp.einsum('bsf,fd->bsd', hidden, down_w, preferred_element_type=F32) + layer_vec[offset:offset + d_model].astype(F32)


def final_norm(residual, lnf_c):
    return layer_norm(residual, lnf_c[0], lnf_c[1]).astype(BF16)


def lse_kernel(h_ref, w_ref, lse_ref, m_ref, s_ref, *, vocab, tile):
    v = pl.program_id(0)
    t = pl.program_id(1)
    n_rows = h_ref.shape[0]
    n_chunk = n_rows // LSE_CHUNK
    last = pl.num_programs(0) - 1

    @pl.when(v == 0)
    def _():
        m_ref[t] = jnp.full(m_ref.shape[1:], -jnp.inf, F32)
        s_ref[t] = jnp.zeros(s_ref.shape[1:], F32)

    def work(masked):
        def product(c):
            return dot(h_ref[c * LSE_CHUNK:(c + 1) * LSE_CHUNK, :], w_ref[...])

        ahead = product(0)
        for c in range(n_chunk):
            logits = ahead
            if c + 1 < n_chunk:
                ahead = product(c + 1)
            part = slice(c * LSE_CHUNK, (c + 1) * LSE_CHUNK)
            if masked:
                ids = lax.broadcasted_iota(jnp.int32, logits.shape, 1) + v * tile
                logits = jnp.where(ids < vocab, logits, -jnp.inf)
            cols = [logits[:, k * 128:(k + 1) * 128] for k in range(tile // 128)]
            m_old = m_ref[t, part, :]
            m_new = m_old
            for x in cols:
                m_new = jnp.maximum(m_new, x)
            s_new = s_ref[t, part, :] * jnp.exp(m_old - jnp.maximum(m_new, LOWEST))
            m_safe = jnp.maximum(m_new, LOWEST)
            for x in cols:
                s_new = s_new + jnp.exp(x - m_safe)
            m_ref[t, part, :] = m_new
            s_ref[t, part, :] = s_new

    @pl.when(v < last)
    def _():
        work(False)

    @pl.when(v == last)
    def _():
        work(True)
        rows = pl.ds(pl.multiple_of(t * n_rows, n_rows), n_rows)
        m_lane = m_ref[t]
        m = jnp.max(m_lane, axis=1, keepdims=True)
        total = jnp.sum(s_ref[t] * jnp.exp(m_lane - m), axis=1, keepdims=True)
        lse_ref[rows, :] = m + jnp.log(total)


def grad_kernel(h_ref, ht_ref, w_ref, lse_ref, tgt_ref, dh_ref, dw_ref, pick_ref, wt_ref, d_ref, *, tile, inv_tokens):
    v = pl.program_id(0)
    t = pl.program_id(1)
    n_rows = h_ref.shape[0]
    n_chunk = n_rows // GRAD_CHUNK

    @pl.when(t == 0)
    def _():
        wt_ref[...] = w_ref[...].T

    @pl.when(v == 0)
    def _():
        dh_ref[t] = jnp.zeros(dh_ref.shape[1:], F32)
        pick_ref[t] = jnp.zeros(pick_ref.shape[1:], F32)

    def product(c):
        return dot(h_ref[c * GRAD_CHUNK:(c + 1) * GRAD_CHUNK, :], w_ref[...])

    ahead = product(0)
    lane = lax.broadcasted_iota(jnp.int32, (GRAD_CHUNK, 128), 1)
    for c in range(n_chunk):
        logits = ahead
        if c + 1 < n_chunk:
            ahead = product(c + 1)
        part = slice(c * GRAD_CHUNK, (c + 1) * GRAD_CHUNK)
        lse = jnp.broadcast_to(lse_ref[part, :], (GRAD_CHUNK, 128))
        place = jnp.broadcast_to(tgt_ref[part, :] - v * tile, (GRAD_CHUNK, 128)) - lane
        pick = pick_ref[t, part, :]
        for k in range(tile // 128):
            shifted = jnp.minimum(logits[:, k * 128:(k + 1) * 128] - lse, 0.0)
            hit = place == k * 128
            pick = jnp.where(hit, shifted, pick)
            prob = jnp.exp(shifted)
            d_ref[part, k * 128:(k + 1) * 128] = jnp.where(hit, prob - 1.0, prob).astype(BF16)
        pick_ref[t, part, :] = pick
        dh_ref[t, part, :] += dot(d_ref[part, :], wt_ref[...])
    term = dot(ht_ref[...], d_ref[...]) * inv_tokens

    @pl.when(t == 0)
    def _():
        dw_ref[...] = term

    @pl.when(t > 0)
    def _():
        dw_ref[...] += term


def head_loss(normed, target_ids, head_t, vocab, inv_tokens):
    n_tok, dm = normed.shape
    padded = head_t.shape[1]
    n_v, n_t = padded // VOCAB_TILE, n_tok // TOKEN_TILE
    flops = 2 * n_tok * padded * dm
    h_spec = pl.BlockSpec((TOKEN_TILE, dm), lambda v, t: (t, 0))
    w_spec = pl.BlockSpec((dm, VOCAB_TILE), lambda v, t: (0, v))
    col_spec = pl.BlockSpec((TOKEN_TILE, 1), lambda v, t: (t, 0))
    full_col = pl.BlockSpec((n_tok, 1), lambda v, t: (0, 0))
    lse = pl.pallas_call(
        functools.partial(lse_kernel, vocab=vocab, tile=VOCAB_TILE),
        grid=(n_v, n_t),
        in_specs=[h_spec, w_spec],
        out_specs=full_col,
        out_shape=jax.ShapeDtypeStruct((n_tok, 1), F32),
        scratch_shapes=[pltpu.VMEM((n_t, TOKEN_TILE, 128), F32), pltpu.VMEM((n_t, TOKEN_TILE, 128), F32)],
        compiler_params=pltpu.CompilerParams(vmem_limit_bytes=BIG_VMEM),
        cost_estimate=pl.CostEstimate(flops=flops, bytes_accessed=head_t.size * 2, transcendentals=0),
        name="head_lse",
    )(normed, head_t)
    d_h, d_w, picked = pl.pallas_call(
        functools.partial(grad_kernel, tile=VOCAB_TILE, inv_tokens=inv_tokens),
        grid=(n_v, n_t),
        in_specs=[h_spec, pl.BlockSpec((dm, TOKEN_TILE), lambda v, t: (0, t)), w_spec, col_spec, col_spec],
        out_specs=[pl.BlockSpec((n_t, TOKEN_TILE, dm), lambda v, t: (0, 0, 0)), w_spec, pl.BlockSpec((n_t, TOKEN_TILE, 128), lambda v, t: (0, 0, 0))],
        out_shape=[jax.ShapeDtypeStruct((n_t, TOKEN_TILE, dm), F32), jax.ShapeDtypeStruct((dm, padded), F32), jax.ShapeDtypeStruct((n_t, TOKEN_TILE, 128), F32)],
        scratch_shapes=[pltpu.VMEM((VOCAB_TILE, dm), BF16), pltpu.VMEM((TOKEN_TILE, VOCAB_TILE), BF16)],
        compiler_params=pltpu.CompilerParams(vmem_limit_bytes=BIG_VMEM),
        cost_estimate=pl.CostEstimate(flops=3 * flops, bytes_accessed=head_t.size * 6, transcendentals=0),
        name="head_grad",
    )(normed, normed.T, head_t, lse, target_ids.reshape(n_tok, 1))
    return d_w, -jnp.sum(picked) * inv_tokens, d_h.reshape(n_tok, dm) * inv_tokens


def gather_kernel(code_ref, table_ref, out_ref, wide_ref, *, width):
    groups = 128 // width
    lane_group = lax.broadcasted_iota(jnp.int32, (1, 128), 1) // width

    @pl.loop(0, out_ref.shape[0] // 16)
    def _(i):
        for j in range(16):
            pos = i * 16 + j
            code = code_ref[0, 0, pos]
            row = table_ref[pl.ds(code >> 2, 1), :]
            wide_ref[pl.ds(pos, 1), :] = jnp.where(lane_group == (code & 3), row, 0.0)

    from_lane = lax.broadcasted_iota(jnp.int32, (128, width), 0) % width
    fold = (from_lane == lax.broadcasted_iota(jnp.int32, (128, width), 1)).astype(F32).astype(BF16)
    out_ref[...] = dot(wide_ref[...].astype(BF16), fold).astype(BF16)


def scatter_kernel(code_ref, dx_ref, out_ref, wide_ref, *accs, width):
    step = pl.program_id(0)
    groups = 128 // width
    lane_group = lax.broadcasted_iota(jnp.int32, (1, 128), 1) // width

    @pl.when(step == 0)
    def _():
        for acc in accs:
            acc[...] = jnp.zeros_like(acc)

    wide_ref[...] = jnp.concatenate([dx_ref[...]] * groups, axis=1)

    @pl.loop(0, dx_ref.shape[0] // (2 * N_ACC))
    def _(i):
        for j in range(2 * N_ACC):
            pos = i * (2 * N_ACC) + j
            code = code_ref[0, 0, pos]
            acc = accs[j % N_ACC]
            row = pl.ds(code >> 2, 1)
            acc[row, :] += jnp.where(lane_group == (code & 3), wide_ref[pl.ds(pos, 1), :], 0.0)

    @pl.when(step == pl.num_programs(0) - 1)
    def _():
        size = accs[0].shape[0]

        @pl.loop(0, size // 128)
        def _(i):
            rows = pl.ds(pl.multiple_of(i * 128, 128), 128)
            total = accs[0][rows, :]
            for acc in accs[1:]:
                total = total + acc[rows, :]
            total = total.T
            for g in range(groups):
                out_ref[:, pl.ds(pl.multiple_of(g * size + i * 128, 128), 128)] = total[g * width:(g + 1) * width, :]


def codes(ids, padded, width, step):
    size = padded * width // 128
    group = (ids >= size).astype(jnp.int32) + (ids >= 2 * size).astype(jnp.int32) + (ids >= 3 * size).astype(jnp.int32)
    code = 4 * (ids - group * size) + group
    return code.reshape(ids.shape[0] // step, 1, step)


def lookup(code, table_t):
    width, padded = table_t.shape
    groups = 128 // width
    assert groups == 4
    size = padded // groups
    steps, _, step = code.shape
    table = jnp.concatenate([table_t[:, g * size:(g + 1) * size] for g in range(groups)], axis=0).astype(F32).T
    return pl.pallas_call(
        functools.partial(gather_kernel, width=width),
        grid=(steps,),
        in_specs=[pl.BlockSpec((1, 1, step), lambda i: (i, 0, 0), memory_space=pltpu.SMEM), pl.BlockSpec((size, 128), lambda i: (0, 0))],
        out_specs=pl.BlockSpec((step, width), lambda i: (i, 0)),
        out_shape=jax.ShapeDtypeStruct((steps * step, width), BF16),
        scratch_shapes=[pltpu.VMEM((step, 128), F32)],
        compiler_params=pltpu.CompilerParams(vmem_limit_bytes=32 * 1024 * 1024),
        name="lookup",
    )(code, table)


def lookup_grad(code, dx, padded):
    width = dx.shape[1]
    groups = 128 // width
    size = padded // groups
    steps, _, step = code.shape
    return pl.pallas_call(
        functools.partial(scatter_kernel, width=width),
        grid=(steps,),
        in_specs=[pl.BlockSpec((1, 1, step), lambda i: (i, 0, 0), memory_space=pltpu.SMEM), pl.BlockSpec((step, width), lambda i: (i, 0))],
        out_specs=pl.BlockSpec((width, padded), lambda i: (0, 0)),
        out_shape=jax.ShapeDtypeStruct((width, padded), F32),
        scratch_shapes=[pltpu.VMEM((step, 128), F32)] + [pltpu.VMEM((size, 128), F32)] * N_ACC,
        compiler_params=pltpu.CompilerParams(vmem_limit_bytes=63 * 1024 * 1024),
        name="lookup_grad",
    )(code, dx)


def adam_update(state, grad, decay):
    moment = BETA_ONE * state[1] + (1.0 - BETA_ONE) * grad
    second = BETA_TWO * state[2] + (1.0 - BETA_TWO) * grad * grad
    m_hat = moment / (1.0 - BETA_ONE ** ADAM_STEP)
    v_hat = second / (1.0 - BETA_TWO ** ADAM_STEP)
    master = state[0] * (1.0 - LEARN_RATE * decay) - LEARN_RATE * m_hat / (jnp.sqrt(v_hat) + ADAM_EPS)
    return jnp.stack([master, moment, second])


def as_rows(x):
    lead = x.shape[0]
    flat = x.reshape(lead, -1)
    size = flat.shape[1]
    total = -(-size // 2048) * 2048
    if total != size:
        flat = jnp.pad(flat, ((0, 0), (0, total - size)))
    return flat.reshape(lead, total // 128, 128)


def pack(parts):
    return jnp.concatenate([as_rows(x) for x in parts], axis=1)


def unpack(packed, shapes):
    out, at = [], 0
    lead = packed.shape[0]
    for shape in shapes:
        size = 1
        for s in shape:
            size *= s
        n_rows = -(-size // 2048) * 16
        piece = packed[:, at:at + n_rows, :].reshape(lead, n_rows * 128)
        out.append(piece[:, :size].reshape((lead,) + tuple(shape)))
        at += n_rows
    return out


def join(piece, axis):
    moved = jnp.moveaxis(piece, 0, axis)
    shape = moved.shape
    return moved.reshape(shape[:axis] + (shape[axis] * shape[axis + 1],) + shape[axis + 2:])


def split(full, axis, n_dev):
    shape = full.shape
    parts = full.reshape(shape[:axis] + (n_dev, shape[axis] // n_dev) + shape[axis + 1:])
    return jnp.moveaxis(parts, axis, 0)


def solution(mesh):
    n_dev = mesh.shape['dp']
    row_spec = P('dp', None)
    state_specs = (P(None, None, 'dp'), P(None, None, 'dp'), P(None, None, 'dp', None, None, None), P(None, None, None, None, 'dp'), P(None, None, 'dp', None), P(None, None, 'dp', None), P(None, None, 'dp'), P(None, None, 'dp'))

    def train_step(token_ids, target_ids, st_wte, st_wpe, st_qkv, st_proj, st_up, st_down, st_vec, st_lnf):
        num_layers = st_qkv.shape[1]
        n_heads, head_dim = st_proj.shape[2], st_proj.shape[3]
        batch_dev, seq_len = token_ids.shape
        vocab = st_wte.shape[1]
        pos_rows = st_wpe.shape[1]
        d_loc = st_wte.shape[2]
        d_model = d_loc * n_dev
        d_ff = st_up.shape[-1]
        n_tok = batch_dev * seq_len
        inv_tokens = 1.0 / (n_tok * n_dev)
        padded = -(-vocab // VOCAB_TILE) * VOCAB_TILE
        axes = (0, 1, 0, 0, 0)
        loc_shapes = ((d_loc, 3 * d_model), (d_model, d_loc), (d_loc, d_ff), (d_ff // n_dev, d_model), (st_vec.shape[2],))

        wte_s = jnp.swapaxes(st_wte, 1, 2)
        wte_t = jnp.pad(wte_s[0].astype(BF16), ((0, 0), (0, padded - vocab)))
        head_t = lax.all_gather(wte_t, 'dp', axis=0, tiled=True)

        pieces = []
        for layer in range(num_layers):
            for state, shape in zip((st_qkv, st_proj, st_up, st_down, st_vec), loc_shapes):
                pieces.append(state[0, layer].astype(BF16).reshape((1,) + shape))
        pieces.append(st_wpe[0, 2:2 + seq_len].astype(BF16)[None])
        pieces.append(st_lnf[0].astype(BF16)[None])
        gathered = lax.all_gather(pack(pieces)[0], 'dp', axis=0, tiled=False)
        full = unpack(gathered, loc_shapes * num_layers + ((seq_len, d_loc), (2, d_loc)))
        weights = []
        for layer in range(num_layers):
            weights.append(tuple(join(x, ax) for x, ax in zip(full[5 * layer:5 * layer + 5], axes)))
        wpe_c = join(full[5 * num_layers], 1)
        lnf_c = join(full[5 * num_layers + 1], 1)

        all_ids = lax.all_gather(token_ids.reshape(-1), 'dp', axis=0, tiled=True)
        code = codes(all_ids, padded, d_loc, 1024)
        found = lookup(code, wte_t)
        found = lax.all_to_all(found, 'dp', split_axis=0, concat_axis=1, tiled=True)
        residual = found.reshape(batch_dev, seq_len, d_model).astype(F32) + wpe_c.astype(F32)
        backs = []
        for layer in range(num_layers):
            residual, back = jax.vjp(functools.partial(block, n_heads=n_heads), residual, weights[layer])
            backs.append(back)
        normed, norm_back = jax.vjp(final_norm, residual, lnf_c)
        grad_head, loss_part, d_normed = head_loss(normed.reshape(n_tok, d_model), target_ids.reshape(n_tok), head_t, vocab, inv_tokens)
        head_loc = lax.psum_scatter(grad_head, 'dp', scatter_dimension=0, tiled=True)
        d_resid, d_lnf = norm_back(d_normed.reshape(residual.shape).astype(BF16))
        layer_loc = [None] * num_layers
        for layer in reversed(range(num_layers)):
            d_resid, d_w = backs[layer](d_resid)
            parts = [split(g.astype(F32), ax, n_dev) for g, ax in zip(d_w, axes)]
            shapes = list(loc_shapes)
            if layer == num_layers - 1:
                parts.append(split(d_lnf.astype(F32), 1, n_dev))
                shapes.append((2, d_loc))
            if layer == 0:
                parts.append(split(jnp.sum(d_resid, axis=0), 1, n_dev))
                shapes.append((seq_len, d_loc))
            summed = jnp.sum(lax.all_to_all(pack(parts), 'dp', split_axis=0, concat_axis=0, tiled=True), axis=0, keepdims=True)
            got = [x[0] for x in unpack(summed, shapes)]
            layer_loc[layer] = got[:5]
            if layer == num_layers - 1:
                lnf_g = got[5]
            if layer == 0:
                pos_g = got[-1]

        dx = lax.all_to_all(d_resid.reshape(n_tok, d_model), 'dp', split_axis=1, concat_axis=0, tiled=True)
        look = lookup_grad(code, dx, padded)
        grads = [(head_loc + look)[:, :vocab], jnp.pad(pos_g, ((2, pos_rows - 2 - seq_len), (0, 0)))]
        state_list = (st_qkv, st_proj, st_up, st_down, st_vec)
        for kind in range(5):
            grads.append(jnp.stack([layer_loc[layer][kind].reshape(state_list[kind].shape[2:]) for layer in range(num_layers)]))
        grads.append(lnf_g)
        local_sq = sum(jnp.sum(grad * grad) for grad in grads)
        sums = lax.psum(jnp.stack([local_sq, loss_part]), 'dp')
        grad_norm = jnp.sqrt(sums[0])
        clip_coef = jnp.minimum(1.0, CLIP_NORM / (grad_norm + 1e-6))
        states = (wte_s, st_wpe, st_qkv, st_proj, st_up, st_down, st_vec, st_lnf)
        new_states = tuple(adam_update(state, grad * clip_coef, decay) for state, grad, decay in zip(states, grads, DECAYS))
        return (sums[1], jnp.swapaxes(new_states[0], 1, 2)) + new_states[1:]

    return jax.shard_map(train_step, mesh=mesh, in_specs=(row_spec, row_spec) + state_specs, out_specs=(P(),) + state_specs, check_vma=False)
```

```python
import functools

import jax
import jax.numpy as jnp
from jax import lax
from jax.experimental import pallas as pl
from jax.experimental.pallas import tpu as pltpu
from jax.sharding import PartitionSpec as P

NORM_EPS = 1e-5
LEARN_RATE = 3e-3
BETA_ONE = 0.9
BETA_TWO = 0.95
ADAM_EPS = 1e-8
WEIGHT_DECAY = 0.1
CLIP_NORM = 1.0
ADAM_STEP = 10
DECAYS = (WEIGHT_DECAY,) * 5 + (0.0, 0.0)
LSE_TILE = 1536
GRAD_TILE = 2304
LCM_TILE = 4608
ADAM_TILE = 4608
TOKEN_TILE = 3072
LSE_CHUNK = 128
GRAD_CHUNK = 256
N_ACC = 8
HEADS_STEP = 4
LOWEST = -3.0e38
FIRST = 0
BIG_VMEM = 60 * 1024 * 1024
F32 = jnp.float32
BF16 = jnp.bfloat16


def layer_norm(residual, gain, bias):
    mean_val = jnp.mean(residual, axis=-1, keepdims=True)
    centered = residual - mean_val
    variance = jnp.mean(centered * centered, axis=-1, keepdims=True)
    return centered * lax.rsqrt(variance + NORM_EPS) * gain.astype(F32) + bias.astype(F32)


def dot(a, b):
    return jnp.dot(a, b, preferred_element_type=F32)


def attn_fwd_kernel(qkv_ref, o_ref, lse_ref, qt_ref, vt_ref, ot_ref, *, seq, dm, hd):
    qt_ref[...] = (qkv_ref[FIRST, :, :dm] * jnp.asarray(hd ** -0.5, BF16)).T
    vt_ref[...] = qkv_ref[FIRST, :, 2 * dm:].T
    half = seq // 2
    per = 128 // hd
    lo, hi = slice(0, half), slice(half, seq)
    row_head = lax.broadcasted_iota(jnp.int32, (128, seq), 0) // hd
    keep = lax.broadcasted_iota(jnp.int32, (half, half), 0) <= lax.broadcasted_iota(jnp.int32, (half, half), 1)
    for slab in range(dm // 128):
        base = slab * 128

        @pl.loop(0, per // HEADS_STEP)
        def _(i):
            todo = []
            for j in range(HEADS_STEP):
                hh = i * HEADS_STEP + j
                qm = jnp.where(row_head == hh, qt_ref[base:base + 128, :], jnp.zeros((), BF16))
                k_lo = qkv_ref[FIRST, lo, dm + base:dm + base + 128]
                k_hi = qkv_ref[FIRST, hi, dm + base:dm + base + 128]
                both = dot(k_lo, qm)
                diag = dot(k_hi, qm[:, hi])
                todo.append((hh, both[:, lo], both[:, hi], diag))
            for hh, s00, s01, s11 in todo:
                rows = pl.ds(pl.multiple_of(base + hh * hd, hd), hd)
                stat = pl.ds(slab * per + hh, 1)
                s00 = jnp.where(keep, s00, -1e30)
                s11 = jnp.where(keep, s11, -1e30)
                m0 = jnp.max(s00, axis=0, keepdims=True)
                e00 = jnp.exp(s00 - m0)
                l0 = jnp.sum(e00, axis=0, keepdims=True)
                m1 = jnp.maximum(jnp.max(s01, axis=0, keepdims=True), jnp.max(s11, axis=0, keepdims=True))
                e01 = jnp.exp(s01 - m1)
                e11 = jnp.exp(s11 - m1)
                l1 = jnp.sum(e01, axis=0, keepdims=True) + jnp.sum(e11, axis=0, keepdims=True)
                inv0, inv1 = 1.0 / l0, 1.0 / l1
                p00 = (e00 * inv0).astype(BF16)
                p01 = (e01 * inv1).astype(BF16)
                p11 = (e11 * inv1).astype(BF16)
                ot_ref[rows, lo] = dot(vt_ref[rows, lo], p00)
                ot_ref[rows, hi] = dot(vt_ref[rows, lo], p01) + dot(vt_ref[rows, hi], p11)
                lse_ref[0, stat, lo] = m0 + jnp.log(l0)
                lse_ref[0, stat, hi] = m1 + jnp.log(l1)

    o_ref[0] = ot_ref[...].T.astype(BF16)


def attn_bwd_kernel(qkv_ref, do_ref, lse_ref, dqkv_ref, qt_ref, kt_ref, dot_ref, dqt_ref, dk_ref, dv_ref, *, seq, dm, hd):
    scale = hd ** -0.5
    qt_ref[...] = (qkv_ref[FIRST, :, :dm] * jnp.asarray(scale, BF16)).T
    kt_ref[...] = qkv_ref[FIRST, :, dm:2 * dm].T
    dot_ref[...] = do_ref[0].T
    dk_ref[...] = jnp.zeros_like(dk_ref)
    dv_ref[...] = jnp.zeros_like(dv_ref)
    half = seq // 2
    per = 128 // hd
    lo, hi = slice(0, half), slice(half, seq)
    zero = jnp.zeros((), BF16)
    row_head = lax.broadcasted_iota(jnp.int32, (128, seq), 0) // hd
    lane_head = lax.broadcasted_iota(jnp.int32, (seq, 128), 1) // hd
    keep = lax.broadcasted_iota(jnp.int32, (half, half), 0) <= lax.broadcasted_iota(jnp.int32, (half, half), 1)
    for slab in range(dm // 128):
        base = slab * 128
        lanes = slice(base, base + 128)
        k_at = slice(dm + base, dm + base + 128)
        v_at = slice(2 * dm + base, 2 * dm + base + 128)

        @pl.loop(0, per // HEADS_STEP)
        def _(i):
            todo = []
            for j in range(HEADS_STEP):
                hh = i * HEADS_STEP + j
                qm = jnp.where(row_head == hh, qt_ref[lanes, :], zero)
                dom = jnp.where(row_head == hh, dot_ref[lanes, :], zero)
                s_lo = dot(qkv_ref[FIRST, lo, k_at], qm)
                s_hi = dot(qkv_ref[FIRST, hi, k_at], qm[:, hi])
                dp_lo = dot(qkv_ref[FIRST, lo, v_at], dom)
                dp_hi = dot(qkv_ref[FIRST, hi, v_at], dom[:, hi])
                todo.append((hh, s_lo, s_hi, dp_lo, dp_hi))
            for hh, s_lo, s_hi, dp_lo, dp_hi in todo:
                rows = pl.ds(pl.multiple_of(base + hh * hd, hd), hd)
                lse = lse_ref[0, pl.ds(slab * per + hh, 1), :]
                q_lane = jnp.where(lane_head == hh, qkv_ref[FIRST, :, lanes], zero)
                do_lane = jnp.where(lane_head == hh, do_ref[0, :, lanes], zero)
                p00 = jnp.exp(jnp.where(keep, s_lo[:, lo], -1e30) - lse[:, lo])
                p01 = jnp.exp(s_lo[:, hi] - lse[:, hi])
                p11 = jnp.exp(jnp.where(keep, s_hi, -1e30) - lse[:, hi])
                w00, w01, w11 = p00 * dp_lo[:, lo], p01 * dp_lo[:, hi], p11 * dp_hi
                delta0 = jnp.sum(w00, axis=0, keepdims=True)
                delta1 = jnp.sum(w01, axis=0, keepdims=True) + jnp.sum(w11, axis=0, keepdims=True)
                ds_lo = jnp.concatenate([(w00 - p00 * delta0).astype(BF16), (w01 - p01 * delta1).astype(BF16)], axis=1)
                ds_hi = (w11 - p11 * delta1).astype(BF16)
                p_lo = jnp.concatenate([p00.astype(BF16), p01.astype(BF16)], axis=1)
                dv_ref[lo, lanes] += dot(p_lo, do_lane)
                dv_ref[hi, lanes] += dot(p11.astype(BF16), do_lane[hi, :])
                dk_ref[lo, lanes] += dot(ds_lo, q_lane)
                dk_ref[hi, lanes] += dot(ds_hi, q_lane[hi, :])
                dq = dot(kt_ref[rows, lo], ds_lo)
                dqt_ref[rows, lo] = dq[:, lo]
                dqt_ref[rows, hi] = dq[:, hi] + dot(kt_ref[rows, hi], ds_hi)

    dqkv_ref[FIRST, :, :dm] = (dqt_ref[...] * scale).T.astype(BF16)
    dqkv_ref[FIRST, :, dm:2 * dm] = (dk_ref[...] * scale).astype(BF16)
    dqkv_ref[FIRST, :, 2 * dm:] = dv_ref[...].astype(BF16)


def attn_fwd_call(qkv, n_heads):
    batch, seq, three = qkv.shape
    dm = three // 3
    flops = 4 * batch * n_heads * seq * seq * 128
    return pl.pallas_call(
        functools.partial(attn_fwd_kernel, seq=seq, dm=dm, hd=dm // n_heads),
        grid=(batch,),
        in_specs=[pl.BlockSpec((1, seq, three), lambda b: (b, 0, 0))],
        out_specs=[pl.BlockSpec((1, seq, dm), lambda b: (b, 0, 0)), pl.BlockSpec((1, n_heads, seq), lambda b: (b, 0, 0))],
        out_shape=[jax.ShapeDtypeStruct((batch, seq, dm), BF16), jax.ShapeDtypeStruct((batch, n_heads, seq), F32)],
        scratch_shapes=[pltpu.VMEM((dm, seq), BF16), pltpu.VMEM((dm, seq), BF16), pltpu.VMEM((dm, seq), F32)],
        cost_estimate=pl.CostEstimate(flops=flops, bytes_accessed=qkv.size * 3, transcendentals=0),
        name="attn_fwd",
    )(qkv)


def attn_bwd_call(qkv, d_o, lse, n_heads):
    batch, seq, three = qkv.shape
    dm = three // 3
    flops = 10 * batch * n_heads * seq * seq * 128
    return pl.pallas_call(
        functools.partial(attn_bwd_kernel, seq=seq, dm=dm, hd=dm // n_heads),
        grid=(batch,),
        in_specs=[pl.BlockSpec((1, seq, three), lambda b: (b, 0, 0)), pl.BlockSpec((1, seq, dm), lambda b: (b, 0, 0)), pl.BlockSpec((1, n_heads, seq), lambda b: (b, 0, 0))],
        out_specs=pl.BlockSpec((1, seq, three), lambda b: (b, 0, 0)),
        out_shape=jax.ShapeDtypeStruct((batch, seq, three), BF16),
        scratch_shapes=[pltpu.VMEM((dm, seq), BF16), pltpu.VMEM((dm, seq), BF16), pltpu.VMEM((dm, seq), BF16), pltpu.VMEM((dm, seq), F32), pltpu.VMEM((seq, dm), F32), pltpu.VMEM((seq, dm), F32)],
        cost_estimate=pl.CostEstimate(flops=flops, bytes_accessed=qkv.size * 6, transcendentals=0),
        name="attn_bwd",
    )(qkv, d_o, lse)


@functools.partial(jax.custom_vjp, nondiff_argnums=(1,))
def attention(qkv, n_heads):
    return attn_fwd_call(qkv, n_heads)[0]


def attention_fwd(qkv, n_heads):
    out, lse = attn_fwd_call(qkv, n_heads)
    return out, (qkv, lse)


def attention_bwd(n_heads, saved, d_o):
    qkv, lse = saved
    return (attn_bwd_call(qkv, d_o.astype(BF16), lse, n_heads),)


attention.defvjp(attention_fwd, attention_bwd)


def block(residual, weights, n_heads):
    qkv_w, proj_w, up_w, down_w, layer_vec = weights
    d_model = residual.shape[-1]
    offset = 4 * d_model + up_w.shape[1]
    ln_par = layer_vec[offset + d_model:].reshape(4, d_model)
    normed_in = layer_norm(residual, ln_par[0], ln_par[1]).astype(BF16)
    qkv = (jnp.einsum('bsd,dn->bsn', normed_in, qkv_w, preferred_element_type=F32) + layer_vec[:3 * d_model].astype(F32)).astype(BF16)
    mixed = attention(qkv, n_heads)
    residual = residual + jnp.einsum('bsd,de->bse', mixed, proj_w, preferred_element_type=F32) + layer_vec[3 * d_model:4 * d_model].astype(F32)
    normed_mid = layer_norm(residual, ln_par[2], ln_par[3]).astype(BF16)
    hidden = jax.nn.relu(jnp.einsum('bsd,df->bsf', normed_mid, up_w, preferred_element_type=F32) + layer_vec[4 * d_model:offset].astype(F32)).astype(BF16)
    return residual + jnp.einsum('bsf,fd->bsd', hidden, down_w, preferred_element_type=F32) + layer_vec[offset:offset + d_model].astype(F32)


def final_norm(residual, lnf_c):
    return layer_norm(residual, lnf_c[0], lnf_c[1]).astype(BF16)


def lse_kernel(h_ref, w_ref, lse_ref, m_ref, s_ref, *, vocab, tile):
    v = pl.program_id(0)
    t = pl.program_id(1)
    n_rows = h_ref.shape[0]
    n_chunk = n_rows // LSE_CHUNK
    last = pl.num_programs(0) - 1

    @pl.when(v == 0)
    def _():
        m_ref[t] = jnp.full(m_ref.shape[1:], -jnp.inf, F32)
        s_ref[t] = jnp.zeros(s_ref.shape[1:], F32)

    def work(masked):
        def product(c):
            return dot(h_ref[c * LSE_CHUNK:(c + 1) * LSE_CHUNK, :], w_ref[...])

        ahead = product(0)
        for c in range(n_chunk):
            logits = ahead
            if c + 1 < n_chunk:
                ahead = product(c + 1)
            part = slice(c * LSE_CHUNK, (c + 1) * LSE_CHUNK)
            if masked:
                ids = lax.broadcasted_iota(jnp.int32, logits.shape, 1) + v * tile
                logits = jnp.where(ids < vocab, logits, -jnp.inf)
            cols = [logits[:, k * 128:(k + 1) * 128] for k in range(tile // 128)]
            m_old = m_ref[t, part, :]
            m_new = m_old
            for x in cols:
                m_new = jnp.maximum(m_new, x)
            s_new = s_ref[t, part, :] * jnp.exp(m_old - jnp.maximum(m_new, LOWEST))
            m_safe = jnp.maximum(m_new, LOWEST)
            for x in cols:
                s_new = s_new + jnp.exp(x - m_safe)
            m_ref[t, part, :] = m_new
            s_ref[t, part, :] = s_new

    @pl.when(v < last)
    def _():
        work(False)

    @pl.when(v == last)
    def _():
        work(True)
        rows = pl.ds(pl.multiple_of(t * n_rows, n_rows), n_rows)
        m_lane = m_ref[t]
        m = jnp.max(m_lane, axis=1, keepdims=True)
        total = jnp.sum(s_ref[t] * jnp.exp(m_lane - m), axis=1, keepdims=True)
        lse_ref[rows, :] = m + jnp.log(total)


def grad_kernel(h_ref, ht_ref, w_ref, lse_ref, tgt_ref, dh_ref, dw_ref, pick_ref, wt_ref, d_ref, *, tile, inv_tokens):
    v = pl.program_id(0)
    t = pl.program_id(1)
    n_rows = h_ref.shape[0]
    n_chunk = n_rows // GRAD_CHUNK

    @pl.when(t == 0)
    def _():
        wt_ref[...] = w_ref[...].T

    @pl.when(v == 0)
    def _():
        dh_ref[t] = jnp.zeros(dh_ref.shape[1:], F32)
        pick_ref[t] = jnp.zeros(pick_ref.shape[1:], F32)

    def product(c):
        return dot(h_ref[c * GRAD_CHUNK:(c + 1) * GRAD_CHUNK, :], w_ref[...])

    ahead = product(0)
    lane = lax.broadcasted_iota(jnp.int32, (GRAD_CHUNK, 128), 1)
    for c in range(n_chunk):
        logits = ahead
        if c + 1 < n_chunk:
            ahead = product(c + 1)
        part = slice(c * GRAD_CHUNK, (c + 1) * GRAD_CHUNK)
        lse = jnp.broadcast_to(lse_ref[part, :], (GRAD_CHUNK, 128))
        place = jnp.broadcast_to(tgt_ref[part, :] - v * tile, (GRAD_CHUNK, 128)) - lane
        pick = pick_ref[t, part, :]
        for k in range(tile // 128):
            shifted = jnp.minimum(logits[:, k * 128:(k + 1) * 128] - lse, 0.0)
            hit = place == k * 128
            pick = jnp.where(hit, shifted, pick)
            prob = jnp.exp(shifted)
            d_ref[part, k * 128:(k + 1) * 128] = jnp.where(hit, prob - 1.0, prob).astype(BF16)
        pick_ref[t, part, :] = pick
        dh_ref[t, part, :] += dot(d_ref[part, :], wt_ref[...])
    term = dot(ht_ref[...], d_ref[...]) * inv_tokens

    @pl.when(t == 0)
    def _():
        dw_ref[...] = term

    @pl.when(t > 0)
    def _():
        dw_ref[...] += term


def head_loss(normed, target_ids, head_t, vocab, inv_tokens):
    n_tok, dm = normed.shape
    padded = head_t.shape[1]
    n_t = n_tok // TOKEN_TILE
    flops = 2 * n_tok * padded * dm
    h_spec = pl.BlockSpec((TOKEN_TILE, dm), lambda v, t: (t, 0))
    w_spec = pl.BlockSpec((dm, GRAD_TILE), lambda v, t: (0, v))
    col_spec = pl.BlockSpec((TOKEN_TILE, 1), lambda v, t: (t, 0))
    full_col = pl.BlockSpec((n_tok, 1), lambda v, t: (0, 0))
    lse = pl.pallas_call(
        functools.partial(lse_kernel, vocab=vocab, tile=LSE_TILE),
        grid=(padded // LSE_TILE, n_t),
        in_specs=[h_spec, pl.BlockSpec((dm, LSE_TILE), lambda v, t: (0, v))],
        out_specs=full_col,
        out_shape=jax.ShapeDtypeStruct((n_tok, 1), F32),
        scratch_shapes=[pltpu.VMEM((n_t, TOKEN_TILE, 128), F32), pltpu.VMEM((n_t, TOKEN_TILE, 128), F32)],
        compiler_params=pltpu.CompilerParams(vmem_limit_bytes=BIG_VMEM),
        cost_estimate=pl.CostEstimate(flops=flops, bytes_accessed=head_t.size * 2, transcendentals=0),
        name="head_lse",
    )(normed, head_t)
    d_h, d_w, picked = pl.pallas_call(
        functools.partial(grad_kernel, tile=GRAD_TILE, inv_tokens=inv_tokens),
        grid=(padded // GRAD_TILE, n_t),
        in_specs=[h_spec, pl.BlockSpec((dm, TOKEN_TILE), lambda v, t: (0, t)), w_spec, col_spec, col_spec],
        out_specs=[pl.BlockSpec((n_t, TOKEN_TILE, dm), lambda v, t: (0, 0, 0)), w_spec, pl.BlockSpec((n_t, TOKEN_TILE, 128), lambda v, t: (0, 0, 0))],
        out_shape=[jax.ShapeDtypeStruct((n_t, TOKEN_TILE, dm), F32), jax.ShapeDtypeStruct((dm, padded), F32), jax.ShapeDtypeStruct((n_t, TOKEN_TILE, 128), F32)],
        scratch_shapes=[pltpu.VMEM((GRAD_TILE, dm), BF16), pltpu.VMEM((TOKEN_TILE, GRAD_TILE), BF16)],
        compiler_params=pltpu.CompilerParams(vmem_limit_bytes=BIG_VMEM),
        cost_estimate=pl.CostEstimate(flops=3 * flops, bytes_accessed=head_t.size * 6, transcendentals=0),
        name="head_grad",
    )(normed, normed.T, head_t, lse, target_ids.reshape(n_tok, 1))
    return d_w, -jnp.sum(picked) * inv_tokens, d_h.reshape(n_tok, dm) * inv_tokens


def gather_kernel(row_ref, mask_ref, table_ref, out_ref, wide_ref, *, width):
    @pl.loop(0, out_ref.shape[0] // 16)
    def _(i):
        for j in range(16):
            pos = i * 16 + j
            wide_ref[pl.ds(pos, 1), :] = table_ref[pl.ds(row_ref[0, 0, pos], 1), :]

    from_lane = lax.broadcasted_iota(jnp.int32, (128, width), 0) % width
    fold = (from_lane == lax.broadcasted_iota(jnp.int32, (128, width), 1)).astype(F32).astype(BF16)
    out_ref[...] = dot(wide_ref[...].astype(BF16) * mask_ref[...], fold).astype(BF16)


def scatter_kernel(row_ref, mask_ref, dx_ref, out_ref, wide_ref, *accs, width):
    step = pl.program_id(0)
    groups = 128 // width

    @pl.when(step == 0)
    def _():
        for acc in accs:
            acc[...] = jnp.zeros_like(acc)

    wide_ref[...] = jnp.concatenate([dx_ref[...]] * groups, axis=1) * mask_ref[...].astype(F32)

    @pl.loop(0, dx_ref.shape[0] // (2 * N_ACC))
    def _(i):
        for j in range(2 * N_ACC):
            pos = i * (2 * N_ACC) + j
            acc = accs[j % N_ACC]
            acc[pl.ds(row_ref[0, 0, pos], 1), :] += wide_ref[pl.ds(pos, 1), :]

    @pl.when(step == pl.num_programs(0) - 1)
    def _():
        size = accs[0].shape[0]

        @pl.loop(0, size // 128)
        def _(i):
            rows = pl.ds(pl.multiple_of(i * 128, 128), 128)
            total = accs[0][rows, :]
            for acc in accs[1:]:
                total = total + acc[rows, :]
            total = total.T
            for g in range(groups):
                out_ref[:, pl.ds(pl.multiple_of(g * size + i * 128, 128), 128)] = total[g * width:(g + 1) * width, :]


def places(ids, padded, width, step):
    size = padded * width // 128
    group = (ids >= size).astype(jnp.int32) + (ids >= 2 * size).astype(jnp.int32) + (ids >= 3 * size).astype(jnp.int32)
    row = ids - group * size
    mask = (group[:, None] == lax.broadcasted_iota(jnp.int32, (1, 128), 1) // width).astype(BF16)
    return row.reshape(ids.shape[0] // step, 1, step), mask


def lookup(row, mask, table_t):
    width, padded = table_t.shape
    groups = 128 // width
    assert groups == 4
    size = padded // groups
    steps, _, step = row.shape
    table = jnp.concatenate([table_t[:, g * size:(g + 1) * size] for g in range(groups)], axis=0).astype(F32).T
    return pl.pallas_call(
        functools.partial(gather_kernel, width=width),
        grid=(steps,),
        in_specs=[pl.BlockSpec((1, 1, step), lambda i: (i, 0, 0), memory_space=pltpu.SMEM), pl.BlockSpec((step, 128), lambda i: (i, 0)), pl.BlockSpec((size, 128), lambda i: (0, 0))],
        out_specs=pl.BlockSpec((step, width), lambda i: (i, 0)),
        out_shape=jax.ShapeDtypeStruct((steps * step, width), BF16),
        scratch_shapes=[pltpu.VMEM((step, 128), F32)],
        compiler_params=pltpu.CompilerParams(vmem_limit_bytes=32 * 1024 * 1024),
        name="lookup",
    )(row, mask, table)


def lookup_grad(row, mask, dx, padded):
    width = dx.shape[1]
    groups = 128 // width
    size = padded // groups
    steps, _, step = row.shape
    return pl.pallas_call(
        functools.partial(scatter_kernel, width=width),
        grid=(steps,),
        in_specs=[pl.BlockSpec((1, 1, step), lambda i: (i, 0, 0), memory_space=pltpu.SMEM), pl.BlockSpec((step, 128), lambda i: (i, 0)), pl.BlockSpec((step, width), lambda i: (i, 0))],
        out_specs=pl.BlockSpec((width, padded), lambda i: (0, 0)),
        out_shape=jax.ShapeDtypeStruct((width, padded), F32),
        scratch_shapes=[pltpu.VMEM((step, 128), F32)] + [pltpu.VMEM((size, 128), F32)] * N_ACC,
        compiler_params=pltpu.CompilerParams(vmem_limit_bytes=63 * 1024 * 1024),
        cost_estimate=pl.CostEstimate(flops=60_000_000_000, bytes_accessed=0, transcendentals=0),
        name="lookup_grad",
    )(row, mask, dx)


def sum_kernel(x_ref, out_ref, got_ref, send_sem, recv_sem, *, n_dev):
    me = lax.axis_index('dp')
    barrier = pltpu.get_barrier_semaphore()
    for k in range(1, n_dev):
        pl.semaphore_signal(barrier, inc=1, device_id=(lax.rem(me + k, n_dev),), device_id_type=pl.DeviceIdType.MESH)
    pl.semaphore_wait(barrier, n_dev - 1)
    copies = []
    for k in range(1, n_dev):
        copy = pltpu.make_async_remote_copy(
            src_ref=x_ref,
            dst_ref=got_ref.at[me],
            send_sem=send_sem.at[k - 1],
            recv_sem=recv_sem.at[k - 1],
            device_id=(lax.rem(me + k, n_dev),),
            device_id_type=pl.DeviceIdType.MESH,
        )
        copy.start()
        copies.append(copy)
    got_ref[me] = x_ref[...]
    for copy in copies:
        copy.wait()
    total = got_ref[0]
    for k in range(1, n_dev):
        total = total + got_ref[k]
    out_ref[...] = total


def device_sums(first, second, n_dev):
    lane = lax.broadcasted_iota(jnp.int32, (8, 128), 1)
    out = pl.pallas_call(
        functools.partial(sum_kernel, n_dev=n_dev),
        in_specs=[pl.BlockSpec(memory_space=pltpu.VMEM)],
        out_specs=pl.BlockSpec(memory_space=pltpu.VMEM),
        out_shape=jax.ShapeDtypeStruct((8, 128), F32),
        scratch_shapes=[pltpu.VMEM((n_dev, 8, 128), F32), pltpu.SemaphoreType.DMA((n_dev - 1,)), pltpu.SemaphoreType.DMA((n_dev - 1,))],
        compiler_params=pltpu.CompilerParams(collective_id=0, has_side_effects=True),
        name="device_sums",
    )(jnp.where(lane == 0, first, jnp.where(lane == 1, second, 0.0)))
    return out[0, 0], out[0, 1]


def adam_parts(master, moment, second, grad, decay):
    moment = BETA_ONE * moment + (1.0 - BETA_ONE) * grad
    second = BETA_TWO * second + (1.0 - BETA_TWO) * grad * grad
    m_hat = moment / (1.0 - BETA_ONE ** ADAM_STEP)
    v_hat = second / (1.0 - BETA_TWO ** ADAM_STEP)
    return master * (1.0 - LEARN_RATE * decay) - LEARN_RATE * m_hat / (jnp.sqrt(v_hat) + ADAM_EPS), moment, second


def adam_update(state, grad, decay):
    return jnp.stack(adam_parts(*state, grad, decay))


def adam_kernel(clip_ref, state_ref, head_ref, look_ref, out_ref):
    grad = (head_ref[...] + look_ref[...]) * clip_ref[0]
    out_ref[...] = jnp.stack(adam_parts(*state_ref[...], grad, WEIGHT_DECAY))


def adam_table(state, head, look, clip_coef):
    kinds, width, vocab = state.shape
    state_spec = pl.BlockSpec((kinds, width, ADAM_TILE), lambda i: (0, 0, i))
    grad_spec = pl.BlockSpec((width, ADAM_TILE), lambda i: (0, i))
    return pl.pallas_call(
        adam_kernel,
        grid=(pl.cdiv(vocab, ADAM_TILE),),
        in_specs=[pl.BlockSpec(memory_space=pltpu.SMEM), state_spec, grad_spec, grad_spec],
        out_specs=state_spec,
        out_shape=jax.ShapeDtypeStruct(state.shape, F32),
        name="adam_table",
    )(clip_coef.reshape(1), state, head, look)


def as_rows(x):
    lead = x.shape[0]
    flat = x.reshape(lead, -1)
    size = flat.shape[1]
    total = -(-size // 2048) * 2048
    if total != size:
        flat = jnp.pad(flat, ((0, 0), (0, total - size)))
    return flat.reshape(lead, total // 128, 128)


def pack(parts):
    return jnp.concatenate([as_rows(x) for x in parts], axis=1)


def unpack(packed, shapes):
    out, at = [], 0
    lead = packed.shape[0]
    for shape in shapes:
        size = 1
        for s in shape:
            size *= s
        n_rows = -(-size // 2048) * 16
        piece = packed[:, at:at + n_rows, :].reshape(lead, n_rows * 128)
        out.append(piece[:, :size].reshape((lead,) + tuple(shape)))
        at += n_rows
    return out


def join(piece, axis):
    moved = jnp.moveaxis(piece, 0, axis)
    shape = moved.shape
    return moved.reshape(shape[:axis] + (shape[axis] * shape[axis + 1],) + shape[axis + 2:])


def split(full, axis, n_dev):
    shape = full.shape
    parts = full.reshape(shape[:axis] + (n_dev, shape[axis] // n_dev) + shape[axis + 1:])
    return jnp.moveaxis(parts, axis, 0)


def solution(mesh):
    n_dev = mesh.shape['dp']
    row_spec = P('dp', None)
    state_specs = tuple(P(*(lead * (None,)), 'dp') for lead in (2, 2, 2, 4, 2, 2, 2, 2))

    def train_step(token_ids, target_ids, st_wte, st_wpe, st_qkv, st_proj, st_up, st_down, st_vec, st_lnf):
        num_layers = st_qkv.shape[1]
        n_heads, head_dim = st_proj.shape[2], st_proj.shape[3]
        batch_dev, seq_len = token_ids.shape
        vocab = st_wte.shape[1]
        pos_rows = st_wpe.shape[1]
        d_loc = st_wte.shape[2]
        d_model = d_loc * n_dev
        d_ff = st_up.shape[-1]
        n_tok = batch_dev * seq_len
        inv_tokens = 1.0 / (n_tok * n_dev)
        padded = -(-vocab // LCM_TILE) * LCM_TILE
        axes = (0, 1, 0, 0, 0)
        loc_shapes = ((d_loc, 3 * d_model), (d_model, d_loc), (d_loc, d_ff), (d_ff // n_dev, d_model), (st_vec.shape[2],))

        wte_s = jnp.swapaxes(st_wte, 1, 2)
        wte_t = jnp.pad(wte_s[0].astype(BF16), ((0, 0), (0, padded - vocab)))

        pieces = []
        for layer in range(num_layers):
            for state, shape in zip((st_qkv, st_proj, st_up, st_down, st_vec), loc_shapes):
                pieces.append(state[0, layer].astype(BF16).reshape((1,) + shape))
        pieces.append(st_wpe[0, 2:2 + seq_len].astype(BF16)[None])
        pieces.append(st_lnf[0].astype(BF16)[None])
        gathered = lax.all_gather(pack(pieces)[0], 'dp', axis=0, tiled=False)
        full = unpack(gathered, loc_shapes * num_layers + ((seq_len, d_loc), (2, d_loc)))
        weights = []
        for layer in range(num_layers):
            weights.append(tuple(join(x, ax) for x, ax in zip(full[5 * layer:5 * layer + 5], axes)))
        wpe_c = join(full[5 * num_layers], 1)
        lnf_c = join(full[5 * num_layers + 1], 1)

        all_ids = lax.all_gather(token_ids.reshape(-1), 'dp', axis=0, tiled=True)
        row, mask = places(all_ids, padded, d_loc, 1024)
        found = lookup(row, mask, wte_t)
        found = lax.all_to_all(found, 'dp', split_axis=0, concat_axis=1, tiled=True)
        wte_late, found = lax.optimization_barrier((wte_t, found))
        head_t = lax.all_gather(wte_late, 'dp', axis=0, tiled=True)
        residual = found.reshape(batch_dev, seq_len, d_model).astype(F32) + wpe_c.astype(F32)
        backs = []
        for layer in range(num_layers):
            residual, back = jax.vjp(functools.partial(block, n_heads=n_heads), residual, weights[layer])
            backs.append(back)
        normed, norm_back = jax.vjp(final_norm, residual, lnf_c)
        grad_head, loss_part, d_normed = head_loss(normed.reshape(n_tok, d_model), target_ids.reshape(n_tok), head_t, vocab, inv_tokens)
        head_loc = lax.psum_scatter(grad_head, 'dp', scatter_dimension=0, tiled=True)
        d_resid, d_lnf = norm_back(d_normed.reshape(residual.shape).astype(BF16))
        layer_loc = [None] * num_layers
        swapped, all_shapes = [], []
        for layer in reversed(range(num_layers)):
            d_resid, d_w = backs[layer](d_resid)
            parts = [split(g.astype(F32), ax, n_dev) for g, ax in zip(d_w, axes)]
            shapes = list(loc_shapes)
            if layer == num_layers - 1:
                parts.append(split(d_lnf.astype(F32), 1, n_dev))
                shapes.append((2, d_loc))
            if layer == 0:
                parts.append(split(jnp.sum(d_resid, axis=0), 1, n_dev))
                shapes.append((seq_len, d_loc))
            packed = pack(parts)
            all_shapes.append(shapes)
            if layer > 0:
                packed, d_resid = lax.optimization_barrier((packed, d_resid))
                swapped.append(lax.all_to_all(packed, 'dp', split_axis=0, concat_axis=0, tiled=True))


        d_resid, swapped[0] = lax.optimization_barrier((d_resid, swapped[0]))
        dx = lax.all_to_all(d_resid.reshape(n_tok, d_model), 'dp', split_axis=1, concat_axis=0, tiled=True)
        packed, dx = lax.optimization_barrier((packed, dx))
        swapped.append(lax.all_to_all(packed, 'dp', split_axis=0, concat_axis=0, tiled=True))
        for layer, pieces_in, shapes in zip(reversed(range(num_layers)), swapped, all_shapes):
            got = [x[0] for x in unpack(jnp.sum(pieces_in, axis=0, keepdims=True), shapes)]
            layer_loc[layer] = got[:5]
            if layer == num_layers - 1:
                lnf_g = got[5]
            if layer == 0:
                pos_g = got[-1]
        look = lookup_grad(row, mask, dx, padded)
        grads = [(head_loc + look)[:, :vocab], jnp.pad(pos_g, ((2, pos_rows - 2 - seq_len), (0, 0)))]
        state_list = (st_qkv, st_proj, st_up, st_down, st_vec)
        for kind in range(5):
            grads.append(jnp.stack([layer_loc[layer][kind].reshape(state_list[kind].shape[2:]) for layer in range(num_layers)]))
        grads.append(lnf_g)
        local_sq = sum(jnp.sum(grad * grad) for grad in grads)
        total_sq, loss = device_sums(local_sq, loss_part, n_dev)
        grad_norm = jnp.sqrt(total_sq)
        clip_coef = jnp.minimum(1.0, CLIP_NORM / (grad_norm + 1e-6))
        new_wte = adam_table(wte_s, head_loc, look, clip_coef)
        states = (st_wpe, st_qkv, st_proj, st_up, st_down, st_vec, st_lnf)
        new_states = tuple(adam_update(state, grad * clip_coef, decay) for state, grad, decay in zip(states, grads[1:], DECAYS))
        return (loss, jnp.swapaxes(new_wte, 1, 2)) + new_states

    return jax.shard_map(train_step, mesh=mesh, in_specs=(row_spec, row_spec) + state_specs, out_specs=(P(),) + state_specs, check_vma=False)
```
